128 devices in a mesh: batch: 32 (over y, z, core), mp: 4 (over x).
Axes of the slice: x: 4, y: 4, z: 4, core: 2. Of those that a mesh axis runs over, the one named last changes fastest.
Arguments:
- init_state: float32 [16384, 256], P(('batch', 'mp')), may hold values from -6 to 6
- brownian: bfloat16 [32, 16384, 256], P(None, ('batch', 'mp')), may hold values from -6 to 6
- step_size: float32 [16384], P(('batch', 'mp')), may hold values from 0.02 to 0.1
- lengths: int32 [16384], P(('batch', 'mp')), may hold values from 1 to 32, as said below
- obs_steps: int32 [16384, 8], P(('batch', 'mp')), may hold values from 1 to 32, as said below
- observed: bfloat16 [16384, 8, 128], P(('batch', 'mp')), may hold values from -6 to 6
- w_in: bfloat16 [256, 1024], P(None, 'mp'), may hold values from -0.375 to 0.375
- b_in: bfloat16 [1024], P('mp'), may hold values from -3 to 3
- w_out: bfloat16 [1024, 256], P('mp'), may hold values from -0.1875 to 0.1875
- b_out: float32 [256], replicated, may hold values from -4 to 4
- decoder: bfloat16 [256, 128], replicated, may hold values from -0.375 to 0.375
- prior_rate: float32 [256], replicated, may hold values from 0.1 to 2
- diffusion: float32 [256], replicated, may hold values from 0.7 to 1.4
Outputs:
- elbo_series: float32 [16384], P(('batch', 'mp'))
- scores: float32 [2], replicated
- grad_w_in: float32 [256, 1024], P(None, 'mp')
- grad_b_in: float32 [1024], P('mp')
- grad_w_out: float32 [1024, 256], P('mp')
- grad_b_out: float32 [256], replicated
- grad_decoder: float32 [256, 128], replicated
- grad_init: float32 [16384, 256], P(('batch', 'mp'))
The draws below stay inside these ranges and needn't reach their ends.
Inputs may be any that keep to these rules, and one draw needn't show every extreme that they name: `lengths`: some series has 32 live steps in every draw. obs_steps[i, j] is at most lengths[i].
All inputs are finite; a program needn't handle non-finite values.
Results may differ from the reference program's by a relative error of at most 0.0019.
Values may be sent and summed in bfloat16 or wider, within the bound.
A program may use at most 64 MiB of HBM per device.

```python
import math
import jax
import jax.numpy as jnp
from jax import lax

L = 256
H = 1024
P_SIZE = 128
OBS = 8
S_STEPS = 32
ROWS_DEV = 128
SERIES = 16384


def length_table(key):
    block_count = SERIES // ROWS_DEV
    key_ceiling, key_choose, key_length, key_place = jax.random.split(jax.random.fold_in(key, 11), 4)
    ceilings = jax.random.randint(key_ceiling, (block_count,), S_STEPS // 4, S_STEPS + 1)
    chosen = jax.random.randint(key_choose, (), 0, block_count)
    ceilings = jnp.where(jnp.arange(block_count) == chosen, S_STEPS, ceilings)
    per_row = jnp.repeat(ceilings, ROWS_DEV, total_repeat_length=SERIES)
    drawn = jax.random.randint(key_length, (SERIES,), 1, per_row + 1)
    places = jax.random.randint(key_place, (block_count,), 0, ROWS_DEV)
    topmost = jnp.arange(SERIES) % ROWS_DEV == jnp.repeat(places, ROWS_DEV, total_repeat_length=SERIES)
    return jnp.where(topmost, per_row, drawn).astype(jnp.int32)


def draw_lengths(key, part):
    return length_table(key)


def draw_obs_steps(key, part):
    table = length_table(key)
    picks = jax.random.randint(jax.random.fold_in(key, 23), (SERIES, OBS), 1, table[:, None] + 1)
    return picks.astype(jnp.int32)


def levels(rng, shape, cuts, smallest, top_value):
    level, own = 1.0, jax.random.fold_in(rng, 6)
    for axis_at, blocks in cuts:
        steps = jnp.exp(jax.random.uniform(jax.random.fold_in(own, axis_at), (blocks,), jnp.float32, smallest / len(cuts), top_value / len(cuts)))
        level = level * jnp.repeat(steps, shape[axis_at] // blocks).reshape([-1 if axis == axis_at else 1 for axis in range(len(shape))])
    return level


def gaussian(own_key, extent, spread, bound, cuts=(), kind=jnp.bfloat16):
    gain = levels(own_key, extent, cuts, -0.22, 0.18) if cuts else 1.0
    values = jax.random.normal(own_key, extent, jnp.float32) * spread * gain
    return jnp.minimum(jnp.maximum(values, -bound), bound).astype(kind)


def setup_inputs(seed: int = 0) -> dict:
    key_list = jax.random.split(jax.random.key(seed), 14)
    init_state = gaussian(key_list[0], (SERIES, L), 1.0, 6.0, ((0, 128),), jnp.float32)
    brownian = gaussian(key_list[1], (S_STEPS, SERIES, L), 1.0, 6.0, ((1, 128),))
    step_size = jnp.clip(jnp.exp(math.log(0.1) - 1.609438 * jax.random.uniform(key_list[2], (SERIES,), jnp.float32) ** levels(key_list[2], (SERIES,), ((0, 128),), -0.2, 0.2)), 0.02, 0.1)
    lengths = draw_lengths(jax.random.fold_in(key_list[13], 71), 0)
    obs_steps = draw_obs_steps(jax.random.fold_in(key_list[13], 71), 0)
    observed = gaussian(key_list[5], (SERIES, OBS, P_SIZE), 1.0, 6.0, ((0, 128),))
    w_in = gaussian(key_list[6], (L, H), L ** -0.5, 0.375, ((1, 4),))
    b_in = gaussian(key_list[7], (H,), 0.5, 3.0, ((0, 4),))
    w_out = gaussian(key_list[8], (H, L), H ** -0.5, 0.1875, ((0, 4),))
    b_out = gaussian(key_list[9], (L,), 1.0, 4.0, (), jnp.float32)
    decoder = gaussian(key_list[10], (L, P_SIZE), L ** -0.5, 0.375)
    prior_rate = jnp.clip(jnp.exp(jax.random.uniform(key_list[11], (L,), jnp.float32, math.log(0.1), math.log(2.0))), 0.1, 2.0)
    diffusion = jnp.clip(jax.random.uniform(key_list[12], (L,), jnp.float32, 0.7, 1.4), 0.7, 1.4)
    return dict(init_state=init_state, brownian=brownian, step_size=step_size, lengths=lengths, obs_steps=obs_steps, observed=observed, w_in=w_in, b_in=b_in, w_out=w_out, b_out=b_out, decoder=decoder, prior_rate=prior_rate, diffusion=diffusion)


def block_terms(block_init, block_noise, block_step, block_lengths, block_obs, block_observed, w_in, b_in, w_out, b_out, decoder, prior_rate, diffusion):
    row_count = block_init.shape[0]
    num_steps = block_noise.shape[0]
    live_mask = (jnp.arange(num_steps, dtype=jnp.int32)[:, None] < block_lengths[None, :]).astype(jnp.float32)
    step_col = block_step[:, None]
    root_col = jnp.sqrt(block_step)[:, None]
    bias_in = b_in.astype(jnp.float32)

    def forward(loop_state, inputs):
        current, kl_sum = loop_state
        increment, live_now = inputs
        activity = jnp.tanh(jnp.dot(current.astype(jnp.bfloat16), w_in, preferred_element_type=jnp.float32) + bias_in).astype(jnp.bfloat16)
        drift_now = jnp.dot(activity, w_out, preferred_element_type=jnp.float32) + b_out
        residual = (drift_now + prior_rate * current) / diffusion
        kl_sum = kl_sum + live_now * 0.5 * block_step * lax.optimization_barrier(jnp.sum(residual * residual, axis=1))
        following = current + live_now[:, None] * (step_col * drift_now + diffusion * root_col * increment.astype(jnp.float32))
        return ((following, kl_sum), (current, activity, residual))
    (last_state, kl_total), (visited, activities, residuals) = lax.scan(forward, (block_init, jnp.zeros((row_count,), jnp.float32)), (block_noise, live_mask))
    trajectory = jnp.concatenate([visited, last_state[None]], axis=0)
    picked = trajectory[block_obs, jnp.arange(row_count, dtype=jnp.int32)[:, None]]
    picked_round = picked.astype(jnp.bfloat16).reshape(-1, picked.shape[2])
    flat_obs = block_observed.reshape(-1, block_observed.shape[2]).astype(jnp.float32)
    misfit = jnp.dot(picked_round, decoder, preferred_element_type=jnp.float32) - flat_obs
    loglik = -0.5 * lax.optimization_barrier(jnp.sum((misfit * misfit).reshape(row_count, -1), axis=1))
    misfit_round = misfit.astype(jnp.bfloat16)
    decoder_grad = jnp.dot(picked_round.T, misfit_round, preferred_element_type=jnp.float32)
    misfit_back = jnp.dot(misfit_round, decoder.T, preferred_element_type=jnp.float32).reshape(row_count, block_obs.shape[1], -1)
    onehot = (block_obs[:, :, None] == jnp.arange(num_steps + 1, dtype=jnp.int32)[None, None, :]).astype(jnp.float32)
    obs_back = jnp.einsum('bjs,bjl->sbl', onehot, misfit_back, precision=lax.Precision.HIGHEST)

    def backward(loop_state, inputs):
        cotangent, sum_w_in, sum_b_in, sum_w_out, sum_b_out = loop_state
        current, activity, residual, live_now, obs_here = inputs
        factor = (live_now * block_step)[:, None]
        scaled = residual / diffusion
        update = factor * (cotangent + scaled)
        update_round = update.astype(jnp.bfloat16)
        activity_value = activity.astype(jnp.float32)
        pre_grad = jnp.dot(update_round, w_out.T, preferred_element_type=jnp.float32) * (1.0 - activity_value * activity_value)
        pre_round = pre_grad.astype(jnp.bfloat16)
        cotangent = cotangent + factor * prior_rate * scaled + jnp.dot(pre_round, w_in.T, preferred_element_type=jnp.float32) + obs_here
        sum_w_in = sum_w_in + jnp.dot(current.astype(jnp.bfloat16).T, pre_round, preferred_element_type=jnp.float32)
        sum_b_in = sum_b_in + lax.optimization_barrier(jnp.sum(pre_grad, axis=0))
        sum_w_out = sum_w_out + jnp.dot(activity.T, update_round, preferred_element_type=jnp.float32)
        sum_b_out = sum_b_out + lax.optimization_barrier(jnp.sum(update, axis=0))
        return ((cotangent, sum_w_in, sum_b_in, sum_w_out, sum_b_out), None)
    start_back = (obs_back[num_steps], jnp.zeros(w_in.shape, jnp.float32), jnp.zeros((w_in.shape[1],), jnp.float32), jnp.zeros(w_out.shape, jnp.float32), jnp.zeros((w_out.shape[1],), jnp.float32))
    (cotangent, sum_w_in, sum_b_in, sum_w_out, sum_b_out), _ = lax.scan(backward, start_back, (visited, activities, residuals, live_mask, obs_back[:num_steps]), reverse=True)
    divisor = (L * block_lengths + P_SIZE * OBS).astype(jnp.float32)
    elbo_rows = (loglik - kl_total) / divisor
    return (elbo_rows, cotangent, jnp.sum(loglik), jnp.sum(kl_total), sum_w_in, sum_b_in, sum_w_out, sum_b_out, decoder_grad)

def reference(init_state, brownian, step_size, lengths, obs_steps, observed, w_in, b_in, w_out, b_out, decoder, prior_rate, diffusion):
    block_count = SERIES // ROWS_DEV
    blocked = (init_state.reshape(block_count, ROWS_DEV, L), jnp.transpose(brownian.reshape(S_STEPS, block_count, ROWS_DEV, L), (1, 0, 2, 3)), step_size.reshape(block_count, ROWS_DEV), lengths.reshape(block_count, ROWS_DEV), obs_steps.reshape(block_count, ROWS_DEV, OBS), observed.reshape(block_count, ROWS_DEV, OBS, P_SIZE))
    zero_totals = (jnp.zeros((L, H), jnp.float32), jnp.zeros((H,), jnp.float32), jnp.zeros((H, L), jnp.float32), jnp.zeros((L,), jnp.float32), jnp.zeros((L, P_SIZE), jnp.float32), jnp.zeros((), jnp.float32), jnp.zeros((), jnp.float32))

    def visit(totals, pieces):
        outcome = block_terms(pieces[0], pieces[1], pieces[2], pieces[3], pieces[4], pieces[5], w_in, b_in, w_out, b_out, decoder, prior_rate, diffusion)
        elbo_rows, init_grad, loglik_sum, kl_sum, sum_w_in, sum_b_in, sum_w_out, sum_b_out, decoder_grad = outcome
        fresh = (sum_w_in, sum_b_in, sum_w_out, sum_b_out, decoder_grad, loglik_sum, kl_sum)
        totals = tuple((first + second for first, second in zip(totals, fresh)))
        return (totals, (elbo_rows, init_grad))
    totals, (elbo_rows, init_grads) = lax.scan(visit, zero_totals, blocked)
    elbo_series = elbo_rows.reshape(SERIES)
    grad_init = init_grads.reshape(SERIES, L)
    scores = jnp.stack([totals[5] / SERIES, totals[6] / SERIES])
    return (elbo_series, scores, totals[0] / SERIES, totals[1] / SERIES, totals[2] / SERIES, totals[3] / SERIES, totals[4] / SERIES, grad_init)
```

```python
import types

import jax
import jax.numpy as jnp
from jax import lax
from jax.experimental import pallas as pl
from jax.experimental.pallas import tpu as pltpu
from jax.sharding import PartitionSpec as P

F32 = jnp.float32
BF16 = jnp.bfloat16


def dot(a, b):
    return jnp.dot(a, b, preferred_element_type=F32)


def fold(value):
    return value.reshape(-1, 8, value.shape[1]).sum(axis=0)


def send(source, target, sems, at, peer):
    return pltpu.make_async_remote_copy(
        src_ref=source,
        dst_ref=target,
        send_sem=sems[0].at[at],
        recv_sem=sems[1].at[at],
        device_id=peer,
        device_id_type=pl.DeviceIdType.MESH,
    )


OPERANDS = (
    "init",
    "noise",
    "step",
    "length",
    "obs",
    "seen",
    "w_in",
    "b_in",
    "w_out",
    "b_out",
    "dec",
    "rate",
    "diff",
)
EXCHANGES = ("w_far", "w_near", "b_far")


def fused_kernel(sizes, r):
    rows, width, steps = sizes.rows, sizes.width, sizes.steps
    seen_count, seen_width = sizes.seen_count, sizes.seen_width
    quarters, planes, total = sizes.quarters, sizes.planes, sizes.total
    mine = lax.axis_index("mp")
    batch = lax.axis_index("batch")
    core = lax.rem(batch, 2)
    other = 1 - core
    place = lax.div(batch, 2)
    sibling = (batch + 1 - 2 * core, mine)

    def quarter_at(d):
        return lax.rem(mine + d, quarters)

    def line_peer(d):
        return (batch, quarter_at(d))

    def place_at(d):
        return lax.rem(place + d, planes)

    def plane_peer(d):
        return (2 * place_at(d) + core, mine)

    far = [2, 1, 3] if quarters == 4 else list(range(1, quarters))

    weights = [
        pltpu.make_async_copy(r.w_in_hbm, r.all_w.at[0, mine], r.load_sem.at[0]),
        pltpu.make_async_copy(r.w_out_hbm, r.all_w.at[1, mine], r.load_sem.at[1]),
        pltpu.make_async_copy(r.b_in_hbm, r.b_own, r.load_sem.at[2]),
    ]
    for copy in weights:
        copy.start()
    loads = []
    for name in OPERANDS:
        if name in ("w_in", "w_out", "b_in"):
            continue
        copy = pltpu.make_async_copy(
            getattr(r, name + "_hbm"), getattr(r, name), r.load_sem.at[3 + len(loads)]
        )
        copy.start()
        loads.append(copy)

    barrier = pltpu.get_barrier_semaphore()
    peers = [sibling] + [line_peer(d) for d in range(1, quarters)]
    peers += [plane_peer(d) for d in range(1, planes)]
    for peer in peers:
        pl.semaphore_signal(barrier, inc=1, device_id=peer, device_id_type=pl.DeviceIdType.MESH)
    for copy in weights:
        copy.wait()
    r.all_b[mine] = jnp.broadcast_to(r.b_own[...].astype(F32), (8, width))
    pl.semaphore_wait(barrier, len(peers))

    sent = []
    for d in far:
        own = r.all_w.at[core, mine]
        copy = send(own, own, r.w_far, d - 1, line_peer(d))
        copy.start()
        sent.append(copy)
    for d in far:
        own = r.all_b.at[mine]
        copy = send(own, own, r.b_far, d - 1, line_peer(d))
        copy.start()
        sent.append(copy)

    def column(row):
        return jnp.broadcast_to(row, (rows, rows)).T

    for copy in loads:
        copy.wait()
    r.dt[...] = column(r.step[...])
    r.root[...] = jnp.sqrt(r.dt[...])
    r.len[...] = column(r.length[...])
    for j in range(seen_count):
        r.obs_wide[j] = column(r.obs[j : j + 1, :])
    r.target[...] = r.seen[...].astype(F32).reshape(r.target.shape)
    r.pick[...] = jnp.zeros_like(r.pick)
    r.kl[...] = jnp.zeros_like(r.kl)
    r.sum_b_in[...] = jnp.zeros_like(r.sum_b_in)
    r.sum_b_out[...] = jnp.zeros_like(r.sum_b_out)
    r.state[...] = r.init[...]
    r.x[0] = r.init[...].astype(BF16)
    dec_t = r.dec[...].T
    r.dec_t[:seen_width, :] = dec_t
    r.dec_t[seen_width:, :] = dec_t

    order = [1, 3, 2] if quarters == 4 else list(range(1, quarters))
    for d in order:
        origin = quarter_at(quarters - d)
        got = r.all_w.at[core, origin]
        send(got, got, r.w_far, d - 1, line_peer(d)).wait_recv()
        copy = send(got, got, r.w_near, d - 1, sibling)
        copy.start()
        sent.append(copy)
    for d in order:
        origin = quarter_at(quarters - d)
        got = r.all_b.at[origin]
        send(got, got, r.b_far, d - 1, line_peer(d)).wait_recv()
        got = r.all_w.at[other, origin]
        send(got, got, r.w_near, d - 1, sibling).wait_recv()
    for copy in sent:
        copy.wait_send()

    def both(value):
        return jnp.concatenate([value] * (width // rows), axis=1)

    def look(k, x):
        seen = dot(x, r.dec[...])
        for j in range(seen_count):
            r.pick[j] = jnp.where(r.obs_wide[j] == k, seen, r.pick[j])

    def turn(k, x):
        r.xt[:, pl.ds(pl.multiple_of(k * rows, rows), rows)] = x.T

    def forward(k, carry):
        x = r.x[k]
        drift = jnp.broadcast_to(r.b_out[...], (rows, width))
        for n in range(quarters):
            act = jnp.tanh(dot(x, r.all_w[0, n]) + r.all_b[n, :1, :]).astype(BF16)
            r.act[n, pl.ds(k * rows, rows), :] = act
            drift = drift + dot(act, r.all_w[1, n])
        state = r.state[...]
        inv = 1.0 / r.diff[...]
        live = k < r.len[...]
        factor = both(jnp.where(live, r.dt[...], 0.0))
        root = both(jnp.where(live, r.root[...], 0.0))
        following = state + (
            factor * drift + r.diff[...] * root * r.noise[k].astype(F32)
        )
        r.state[...] = following
        r.x[k + 1] = following.astype(BF16)
        residual = (drift + r.rate[...] * state) * inv
        r.kl[...] += factor * residual * residual
        r.scaled[k] = residual * inv
        turn(k, x)
        look(k, x)
        which = lax.rem(k, 2 * quarters)
        tensor, n = lax.div(which, quarters), lax.rem(which, quarters)
        r.all_t[tensor, n] = r.all_w[tensor, n].T
        return carry

    lax.fori_loop(0, steps, forward, 0)
    look(steps, r.x[steps])
    turn(steps, r.x[steps])

    square = jnp.zeros((rows, seen_width), F32)
    for j in range(seen_count):
        misfit = r.pick[j] - r.target[pl.ds(j, rows, stride=seen_count), :]
        square = square + misfit * misfit
        r.pick[j] = misfit.astype(BF16).astype(F32)
    loglik = -0.5 * jnp.sum(square.T, axis=0, keepdims=True)
    kl_half = r.kl[:, :rows]
    for part in range(1, width // rows):
        kl_half = kl_half + r.kl[:, part * rows : (part + 1) * rows]
    kl_row = 0.5 * jnp.sum(kl_half.T, axis=0, keepdims=True)
    divisor = (width * r.length[...] + seen_width * seen_count).astype(F32)
    r.elbo_out[...] = (loglik - kl_row) / divisor

    def observe(t):
        spread = jnp.zeros((rows, seen_width), F32)
        for j in range(seen_count):
            spread = spread + jnp.where(r.obs_wide[j] == t, r.pick[j], 0.0)
        high = spread.astype(BF16)
        low = (spread - high.astype(F32)).astype(BF16)
        pair = jnp.concatenate([high, low], axis=1)
        r.miss[pl.ds(t * rows, rows), :] = pair
        r.obs_back[...] = dot(pair, r.dec_t[...])

    observe(steps)
    r.cot[...] = jnp.zeros_like(r.cot)

    def backward(index, carry):
        k = steps - 1 - index
        cot = r.cot[...] + r.obs_back[...]
        scaled = r.scaled[k]
        factor = both(jnp.where(k < r.len[...], r.dt[...], 0.0))
        update = factor * (cot + scaled)
        rounded = update.astype(BF16)
        cot = cot + factor * r.rate[...] * scaled
        for n in range(quarters):
            act = r.act[n, pl.ds(k * rows, rows), :].astype(F32)
            pre = dot(rounded, r.all_t[1, n]) * (1.0 - act * act)
            pre_round = pre.astype(BF16)
            cot = cot + dot(pre_round, r.all_t[0, n])
            r.pre[n, pl.ds(k * rows, rows), :] = pre_round
            r.sum_b_in[n] += fold(pre)
        r.cot[...] = cot
        r.ut[:, pl.ds(pl.multiple_of(k * rows, rows), rows)] = rounded.T
        r.sum_b_out[...] += fold(update)
        observe(k)
        return carry

    lax.fori_loop(0, steps, backward, 0)
    r.cot_out[...] = r.cot[...]

    for n in range(quarters):
        r.tail[n : n + 1, :] = jnp.sum(r.sum_b_in[n], axis=0, keepdims=True)
    r.tail[quarters : quarters + 1, :] = jnp.sum(r.sum_b_out[...], axis=0, keepdims=True)
    r.tail[quarters + 1 : quarters + 2, :rows] = loglik
    r.tail[quarters + 1 : quarters + 2, rows : 2 * rows] = kl_row
    r.tail[quarters + 2 :, :] = jnp.zeros((r.tail.shape[0] - quarters - 2, width), F32)
    tail_near = send(r.tail, r.tail_sib, r.near, 0, sibling)
    tail_near.start()
    waits = [tail_near]
    dec_grad = dot(r.xt[:, rows:], r.miss[rows:, :])
    dec_grad = dec_grad[:, :seen_width] + dec_grad[:, seen_width:]
    r.dec_part[...] = dec_grad.reshape(r.dec_part.shape)
    dec_near = send(r.dec_part.at[other], r.dec_sib, r.near, 1, sibling)
    dec_near.start()
    waits.append(dec_near)
    dec_rows = r.dec_sum.shape[1]

    def chunk(i, d):
        n = quarter_at(d)
        r.grad[i, 0] = dot(r.xt[:, : steps * rows], r.pre[n])
        r.grad[i, 1] = dot(r.ut[...], r.act[n]).T
        copy = send(r.grad.at[i, other], r.grad_sib.at[i], r.near, 3 + i, sibling)
        copy.start()
        waits.append(copy)
        return copy

    def joined(i, copy):
        copy.wait_recv()
        return r.grad[i, core] + r.grad_sib[i]

    def pass_on(i, d, copy):
        r.line_out[i] = joined(i, copy).astype(BF16)
        moved = send(r.line_out.at[i], r.line_in.at[i], r.line, i, line_peer(d))
        moved.start()
        waits.append(moved)
        return moved

    passed = []
    for i, d in enumerate(far):
        near = chunk(i, d)
        if i == 0:
            tail_near.wait_recv()
            r.tail_sum[...] = r.tail[...] + r.tail_sib[...]
            dec_near.wait_recv()
            r.dec_sum[...] = (r.dec_part[core] + r.dec_sib[...]).reshape(r.dec_sum.shape)
            tail_plane, dec_plane = [], []
            for e in range(1, planes):
                copy = send(r.tail_sum, r.tail_in.at[e - 1], r.tail_plane, e - 1, plane_peer(e))
                copy.start()
                tail_plane.append(copy)
                copy = send(
                    r.dec_sum.at[place_at(e)],
                    r.dec_in.at[e - 1],
                    r.dec_plane,
                    e - 1,
                    plane_peer(e),
                )
                copy.start()
                dec_plane.append(copy)
            waits += tail_plane + dec_plane
        if i == 1:
            value = r.tail_sum[...]
            for e in range(1, planes):
                tail_plane[e - 1].wait_recv()
                value = value + r.tail_in[e - 1]
            r.tail_line[...] = value
            value = r.dec_sum[place]
            for e in range(1, planes):
                dec_plane[e - 1].wait_recv()
                value = value + r.dec_in[e - 1]
            r.dec_line[...] = value
            tail_far, dec_far = [], []
            for e in range(1, quarters):
                copy = send(
                    r.tail_line, r.tail_line_in.at[e - 1], r.tail_far, e - 1, line_peer(e)
                )
                copy.start()
                tail_far.append(copy)
                copy = send(r.dec_line, r.dec_line_in.at[e - 1], r.dec_far, e - 1, line_peer(e))
                copy.start()
                dec_far.append(copy)
            waits += tail_far + dec_far
        if i == 2:
            value = r.tail_line[...]
            for e in range(1, quarters):
                tail_far[e - 1].wait_recv()
                value = value + r.tail_line_in[e - 1]
            r.tail_total[...] = value
            value = r.dec_line[...]
            for e in range(1, quarters):
                dec_far[e - 1].wait_recv()
                value = value + r.dec_line_in[e - 1]
            r.dec_all[core, place] = value / total
            own = r.dec_all.at[core, place]
            for e in range(1, planes):
                copy = send(own, own, r.dec_spread, e - 1, plane_peer(e))
                copy.start()
                waits.append(copy)
        passed.append(pass_on(i, d, near))

    last = len(far)
    near = chunk(last, 0)
    for e in range(1, planes):
        got = r.dec_all.at[core, place_at(planes - e)]
        send(got, got, r.dec_spread, e - 1, plane_peer(e)).wait_recv()
    dec_hand = send(r.dec_all.at[core], r.dec_all.at[core], r.near, 2, sibling)
    dec_hand.start()
    value = joined(last, near)
    for i in range(last):
        passed[i].wait_recv()
        value = value + r.line_in[i].astype(F32)
    r.full[...] = value
    r.plane_out[...] = value.astype(BF16).reshape(r.plane_out.shape)
    plane = []
    for e in range(1, planes):
        copy = send(
            r.plane_out.at[place_at(e)], r.plane_in.at[e - 1], r.plane, e - 1, plane_peer(e)
        )
        copy.start()
        plane.append(copy)
    waits += plane
    piece = width // planes

    def rows_of(tensor, owner):
        return r.res_out.at[tensor, pl.ds(pl.multiple_of(owner * piece, piece), piece), :]

    value = r.full[pl.ds(pl.multiple_of(place * piece, piece), piece), :]
    for e in range(1, planes):
        plane[e - 1].wait_recv()
        value = value + r.plane_in[e - 1].astype(F32)
    r.res_out[core, pl.ds(pl.multiple_of(place * piece, piece), piece), :] = value / total
    own = rows_of(core, place)
    for e in range(1, planes):
        copy = send(own, own, r.spread, e - 1, plane_peer(e))
        copy.start()
        waits.append(copy)
    copy = send(own, own, r.hand, 0, sibling)
    copy.start()
    waits.append(copy)
    for e in range(1, planes):
        got = rows_of(core, place_at(planes - e))
        send(got, got, r.spread, e - 1, plane_peer(e)).wait_recv()
        copy = send(got, got, r.hand, e, sibling)
        copy.start()
        waits.append(copy)
    got = r.dec_all.at[other]
    send(got, got, r.near, 2, sibling).wait_recv()
    r.dec_out[...] = r.dec_all[...].reshape(r.dec_out.shape)
    scale = 1.0 / total
    r.tail_out[0:1, :] = r.tail_total[pl.ds(mine, 1), :] * scale
    r.tail_out[1:3, :] = r.tail_total[quarters : quarters + 2, :] * scale
    r.tail_out[3:, :] = jnp.zeros((r.tail_out.shape[0] - 3, width), F32)
    for copy in waits:
        copy.wait_send()
    dec_hand.wait_send()
    for e in range(planes):
        got = rows_of(other, place_at(planes - e) if e else place)
        send(got, got, r.hand, e, sibling).wait_recv()


def fused(sizes, operands):
    rows, width, steps = sizes.rows, sizes.width, sizes.steps
    count, seen_width = sizes.seen_count, sizes.seen_width
    quarters, planes = sizes.quarters, sizes.planes
    piece = width // planes
    dec_rows = width // 2 // planes
    outs = {
        "elbo_out": ((1, rows), F32),
        "res_out": ((2, width, width), F32),
        "tail_out": ((8, width), F32),
        "dec_out": ((width, seen_width), F32),
        "cot_out": ((rows, width), F32),
    }
    arrays = {
        "x": ((steps + 1, rows, width), BF16),
        "xt": ((width, (steps + 1) * rows), BF16),
        "ut": ((width, steps * rows), BF16),
        "act": ((quarters, steps * rows, width), BF16),
        "pre": ((quarters, steps * rows, width), BF16),
        "scaled": ((steps, rows, width), F32),
        "pick": ((count, rows, seen_width), F32),
        "obs_wide": ((count, rows, rows), jnp.int32),
        "dt": ((rows, rows), F32),
        "root": ((rows, rows), F32),
        "len": ((rows, rows), jnp.int32),
        "state": ((rows, width), F32),
        "kl": ((rows, width), F32),
        "cot": ((rows, width), F32),
        "obs_back": ((rows, width), F32),
        "sum_b_in": ((quarters, 8, width), F32),
        "sum_b_out": ((8, width), F32),
        "miss": (((steps + 1) * rows, 2 * seen_width), BF16),
        "target": ((rows * count, seen_width), F32),
        "all_w": ((2, quarters, width, width), BF16),
        "all_t": ((2, quarters, width, width), BF16),
        "all_b": ((quarters, 8, width), F32),
        "b_own": (sizes.b_shape, BF16),
        "dec_t": ((2 * seen_width, width), BF16),
        "tail": ((8, width), F32),
        "tail_sib": ((8, width), F32),
        "tail_sum": ((8, width), F32),
        "tail_in": ((planes - 1, 8, width), F32),
        "tail_line": ((8, width), F32),
        "tail_total": ((8, width), F32),
        "tail_line_in": ((quarters - 1, 8, width), F32),
        "dec_part": ((2, width // 2, seen_width), F32),
        "dec_sib": ((width // 2, seen_width), F32),
        "dec_sum": ((planes, dec_rows, seen_width), F32),
        "dec_in": ((planes - 1, dec_rows, seen_width), F32),
        "dec_line": ((dec_rows, seen_width), F32),
        "dec_line_in": ((quarters - 1, dec_rows, seen_width), F32),
        "dec_all": ((2, planes, dec_rows, seen_width), F32),
        "grad": ((quarters, 2, width, width), F32),
        "grad_sib": ((quarters, width, width), F32),
        "line_out": ((quarters - 1, width, width), BF16),
        "line_in": ((quarters - 1, width, width), BF16),
        "full": ((width, width), F32),
        "plane_out": ((planes, piece, width), BF16),
        "plane_in": ((planes - 1, piece, width), BF16),
    }
    for name, value in zip(OPERANDS, operands):
        if name not in ("w_in", "w_out", "b_in"):
            arrays[name] = (value.shape, value.dtype)
    links = {
        "w_far": quarters - 1,
        "w_near": quarters - 1,
        "b_far": quarters - 1,
        "near": 3 + quarters,
        "line": quarters - 1,
        "tail_plane": planes - 1,
        "dec_plane": planes - 1,
        "tail_far": quarters - 1,
        "dec_far": quarters - 1,
        "dec_spread": planes - 1,
        "plane": planes - 1,
        "spread": planes - 1,
        "hand": planes,
    }
    scratch = [pltpu.VMEM(shape, dtype) for shape, dtype in arrays.values()]
    for number in links.values():
        scratch += [pltpu.SemaphoreType.DMA((number,))] * 2
    scratch.append(pltpu.SemaphoreType.DMA((len(OPERANDS),)))

    def body(*refs):
        refs = list(refs)
        r = types.SimpleNamespace()
        for name in OPERANDS:
            setattr(r, name + "_hbm", refs.pop(0))
        for name in list(outs) + list(arrays):
            setattr(r, name, refs.pop(0))
        for name in links:
            setattr(r, name, (refs.pop(0), refs.pop(0)))
        r.load_sem = refs.pop(0)
        fused_kernel(sizes, r)

    return pl.pallas_call(
        body,
        out_shape=[jax.ShapeDtypeStruct(shape, dtype) for shape, dtype in outs.values()],
        in_specs=[pl.BlockSpec(memory_space=pltpu.HBM)] * len(OPERANDS),
        out_specs=[pl.BlockSpec(memory_space=pltpu.VMEM)] * len(outs),
        scratch_shapes=scratch,
        compiler_params=pltpu.CompilerParams(
            collective_id=0, has_side_effects=True, vmem_limit_bytes=60 * 1024 * 1024
        ),
        name="fused",
    )(*operands)


def finish_kernel(half, res_ref, tail_ref, dec_in, cot_in, elbo_in, w_in, w_out, b_in, b_out, dec, scores, cot, elbo):
    w_in[...] = res_ref[0]
    w_out[...] = res_ref[1]
    b_in[...] = tail_ref[0:1, :]
    b_out[...] = tail_ref[1:2, :]
    scores[:, 0:1] = jnp.sum(tail_ref[2:3, :half], axis=1, keepdims=True)
    scores[:, 1:2] = jnp.sum(tail_ref[2:3, half : 2 * half], axis=1, keepdims=True)
    dec[...] = dec_in[...]
    cot[...] = cot_in[...]
    elbo[...] = elbo_in[...]


def finish(rows, res, tail, dec, cot, elbo):
    width, seen_width = dec.shape
    shapes = [
        (width, width),
        (width, width),
        (1, width),
        (1, width),
        dec.shape,
        (1, 2),
        cot.shape,
        elbo.shape,
    ]

    def body(*refs):
        finish_kernel(rows, *refs)

    vmem = pl.BlockSpec(memory_space=pltpu.VMEM)
    return pl.pallas_call(
        body,
        out_shape=[jax.ShapeDtypeStruct(shape, F32) for shape in shapes],
        in_specs=[vmem] * 5,
        out_specs=[vmem] * len(shapes),
        compiler_params=pltpu.CompilerParams(vmem_limit_bytes=8 * 1024 * 1024),
        name="finish",
    )(res, tail, dec, cot, elbo)


def on_device(
    init_state,
    brownian,
    step_size,
    lengths,
    obs_steps,
    observed,
    w_in,
    b_in,
    w_out,
    b_out,
    decoder,
    prior_rate,
    diffusion,
):
    rows, width = init_state.shape
    quarters = lax.axis_size("mp")
    members = lax.axis_size("batch")
    sizes = types.SimpleNamespace(
        rows=rows,
        width=width,
        steps=brownian.shape[0],
        seen_count=observed.shape[1],
        seen_width=observed.shape[2],
        quarters=quarters,
        planes=members // 2,
        total=rows * members * quarters,
        b_shape=(1, b_in.shape[0]),
    )
    elbo, res, tail, dec, cot = fused(
        sizes,
        (
            init_state,
            brownian,
            step_size[None, :],
            lengths[None, :],
            obs_steps.T,
            observed,
            w_in,
            b_in[None, :],
            w_out,
            b_out[None, :],
            decoder,
            prior_rate[None, :],
            diffusion[None, :],
        ),
    )
    own_w_in, own_w_out, own_b_in, b_out_grad, dec_grad, scores, cot, elbo = finish(
        rows, res, tail, dec, cot, elbo
    )
    return (
        elbo[0],
        scores[0],
        own_w_in,
        own_b_in[0],
        own_w_out,
        b_out_grad[0],
        dec_grad,
        cot,
    )


def solution(mesh):
    both = ("batch", "mp")
    placed = (
        P(both, None),
        P(None, both, None),
        P(both),
        P(both),
        P(both, None),
        P(both, None, None),
        P(None, "mp"),
        P("mp"),
        P("mp", None),
        P(),
        P(),
        P(),
        P(),
    )
    return jax.shard_map(
        on_device,
        mesh=mesh,
        in_specs=placed,
        out_specs=(
            P(both),
            P(),
            P(None, "mp"),
            P("mp"),
            P("mp", None),
            P(),
            P(),
            P(both, None),
        ),
        check_vma=False,
    )
```

```python
import types

import jax
import jax.numpy as jnp
from jax import lax
from jax.experimental import pallas as pl
from jax.experimental.pallas import tpu as pltpu
from jax.sharding import PartitionSpec as P

UNROLL = 4
F32 = jnp.float32
BF16 = jnp.bfloat16


def dot(a, b):
    return jnp.dot(a, b, preferred_element_type=F32)


def fold(value):
    return value.reshape(-1, 8, value.shape[1]).sum(axis=0)


def send(source, target, sems, at, peer):
    return pltpu.make_async_remote_copy(
        src_ref=source,
        dst_ref=target,
        send_sem=sems[0].at[at],
        recv_sem=sems[1].at[at],
        device_id=peer,
        device_id_type=pl.DeviceIdType.MESH,
    )


OPERANDS = (
    "init",
    "noise",
    "step",
    "length",
    "obs",
    "seen",
    "w_in",
    "b_in",
    "w_out",
    "b_out",
    "dec",
    "rate",
    "diff",
)
EXCHANGES = ("w_far", "w_near", "b_far")


def fused_kernel(sizes, r):
    rows, width, steps = sizes.rows, sizes.width, sizes.steps
    seen_count, seen_width = sizes.seen_count, sizes.seen_width
    quarters, planes, total = sizes.quarters, sizes.planes, sizes.total
    mine = lax.axis_index("mp")
    batch = lax.axis_index("batch")
    core = lax.rem(batch, 2)
    other = 1 - core
    place = lax.div(batch, 2)
    sibling = (batch + 1 - 2 * core, mine)

    def quarter_at(d):
        return lax.rem(mine + d, quarters)

    def line_peer(d):
        return (batch, quarter_at(d))

    def place_at(d):
        return lax.rem(place + d, planes)

    def plane_peer(d):
        return (2 * place_at(d) + core, mine)

    def arrived(whole, sems):
        send(whole, whole, sems, 0, sibling).wait_recv()

    def departed(whole, sems):
        send(whole, whole, sems, 0, sibling).wait_send()

    far = [2, 1, 3] if quarters == 4 else list(range(1, quarters))

    weights = [
        pltpu.make_async_copy(r.w_in_hbm, r.all_w.at[0, mine], r.load_sem.at[0]),
        pltpu.make_async_copy(r.w_out_hbm, r.all_w.at[1, mine], r.load_sem.at[1]),
        pltpu.make_async_copy(r.b_in_hbm, r.b_own, r.load_sem.at[2]),
    ]
    for copy in weights:
        copy.start()
    loads = []
    for name in OPERANDS:
        if name in ("w_in", "w_out", "b_in"):
            continue
        copy = pltpu.make_async_copy(
            getattr(r, name + "_hbm"), getattr(r, name), r.load_sem.at[3 + len(loads)]
        )
        copy.start()
        loads.append(copy)

    barrier = pltpu.get_barrier_semaphore()
    peers = [sibling] + [line_peer(d) for d in range(1, quarters)]
    peers += [plane_peer(d) for d in range(1, planes)]
    for peer in peers:
        pl.semaphore_signal(barrier, inc=1, device_id=peer, device_id_type=pl.DeviceIdType.MESH)
    for copy in weights:
        copy.wait()
    r.all_b[mine] = jnp.broadcast_to(r.b_own[...].astype(F32)[None, :], (8, width))
    pl.semaphore_wait(barrier, len(peers))

    sent = []
    for d in far:
        own = r.all_w.at[core, mine]
        copy = send(own, own, r.w_far, d - 1, line_peer(d))
        copy.start()
        sent.append(copy)
    for d in far:
        own = r.all_b.at[mine]
        send(own, own, r.b_far, 0, line_peer(d)).start()

    def column(row):
        return jnp.broadcast_to(row, (rows, rows)).T

    for copy in loads:
        copy.wait()
    r.dt[...] = column(r.step[...])
    r.root[...] = jnp.sqrt(r.dt[...])
    r.len[...] = column(r.length[...])
    for j in range(seen_count):
        r.obs_wide[j] = column(r.obs[j : j + 1, :])
    r.target[...] = r.seen[...].astype(F32).reshape(r.target.shape)
    r.pick[...] = jnp.zeros_like(r.pick)
    r.kl[...] = jnp.zeros_like(r.kl)
    r.sum_b_in[...] = jnp.zeros_like(r.sum_b_in)
    r.sum_b_out[...] = jnp.zeros_like(r.sum_b_out)
    r.state[...] = r.init[...]
    r.ones[...] = jnp.ones_like(r.ones)
    dec_t = r.dec[...].T
    r.dec_t[:seen_width, :] = dec_t
    r.dec_t[seen_width:, :] = dec_t

    order = [1, 3, 2] if quarters == 4 else list(range(1, quarters))
    for d in order:
        origin = quarter_at(quarters - d)
        got = r.all_w.at[core, origin]
        send(got, got, r.w_far, d - 1, line_peer(d)).wait_recv()
        send(got, got, r.w_near, 0, sibling).start()
    arrived(r.all_b.at[pl.ds(0, quarters - 1)], r.b_far)
    arrived(r.all_w.at[other, pl.ds(0, quarters - 1)], r.w_near)
    departed(r.all_b.at[pl.ds(0, quarters - 1)], r.b_far)
    departed(r.all_w.at[core, pl.ds(0, quarters - 1)], r.w_near)
    for copy in sent:
        copy.wait_send()

    def both(value):
        return jnp.concatenate([value] * (width // rows), axis=1)

    def look(k, x):
        seen = dot(x, r.dec[...])
        for j in range(seen_count):
            r.pick[j] = jnp.where(r.obs_wide[j] == k, seen, r.pick[j])

    def turn(k, x):
        r.xt[:, pl.ds(pl.multiple_of(k * rows, rows), rows)] = x.T

    def advance(k, state):
        x = state.astype(BF16)
        drift = jnp.broadcast_to(r.b_out[...], (rows, width))
        for n in range(quarters):
            act = jnp.tanh(dot(x, r.all_w[0, n]) + r.all_b[n, :1, :]).astype(BF16)
            r.act[n, pl.ds(k * rows, rows), :] = act
            drift = drift + dot(act, r.all_w[1, n])
        inv = 1.0 / r.diff[...]
        live = k < r.len[...]
        factor = both(jnp.where(live, r.dt[...], 0.0))
        root = both(jnp.where(live, r.root[...], 0.0))
        following = state + (
            factor * drift + r.diff[...] * root * r.noise[k].astype(F32)
        )
        residual = (drift + r.rate[...] * state) * inv
        r.kl[...] += factor * residual * residual
        r.scaled[k] = residual * inv
        turn(k, x)
        look(k, x)
        which = lax.rem(k, 2 * quarters)
        tensor, n = lax.div(which, quarters), lax.rem(which, quarters)
        r.all_t[tensor, n] = r.all_w[tensor, n].T
        return following

    def forward(index, carry):
        state = r.state[...]
        for u in range(sizes.unroll):
            state = advance(index * sizes.unroll + u, state)
        r.state[...] = state
        return carry

    lax.fori_loop(0, steps // sizes.unroll, forward, 0)
    final = r.state[...].astype(BF16)
    look(steps, final)
    turn(steps, final)

    square = jnp.zeros((rows, seen_width), F32)
    for j in range(seen_count):
        misfit = r.pick[j] - r.target[pl.ds(j, rows, stride=seen_count), :]
        square = square + misfit * misfit
        r.pick[j] = misfit.astype(BF16).astype(F32)
    loglik = -0.5 * jnp.sum(square.T, axis=0, keepdims=True)
    kl_half = r.kl[:, :rows]
    for part in range(1, width // rows):
        kl_half = kl_half + r.kl[:, part * rows : (part + 1) * rows]
    kl_row = 0.5 * jnp.sum(kl_half.T, axis=0, keepdims=True)
    divisor = (width * r.length[...] + seen_width * seen_count).astype(F32)
    r.elbo[...] = (loglik - kl_row) / divisor

    def observe(t):
        spread = jnp.zeros((rows, seen_width), F32)
        for j in range(seen_count):
            spread = spread + jnp.where(r.obs_wide[j] == t, r.pick[j], 0.0)
        high = spread.astype(BF16)
        low = (spread - high.astype(F32)).astype(BF16)
        pair = jnp.concatenate([high, low], axis=1)
        r.miss[pl.ds(t * rows, rows), :] = pair
        return dot(pair, r.dec_t[...])

    r.cot[...] = observe(steps)

    def joint(parts):
        half = len(parts) // 2
        first, second = sum(parts[1:half], parts[0]), sum(parts[half + 1 :], parts[half])
        return first * r.ones[...] + second

    def retreat(k, cot):
        scaled = r.scaled[k]
        factor = both(jnp.where(k < r.len[...], r.dt[...], 0.0))
        update = factor * (cot + scaled)
        rounded = update.astype(BF16)
        cot = cot + factor * r.rate[...] * scaled
        cot = cot + observe(k)
        inner = [dot(rounded, r.all_t[1, n]) for n in range(quarters)]
        pres = []
        for n in range(quarters):
            act = r.act[n, pl.ds(k * rows, rows), :].astype(F32)
            pre = inner[n] * (1.0 - act * act)
            pre_round = pre.astype(BF16)
            pres.append(pre_round)
            r.pre[n, pl.ds(k * rows, rows), :] = pre_round
            r.sum_b_in[n] += fold(pre)
        r.ut[:, pl.ds(pl.multiple_of(k * rows, rows), rows)] = rounded.T
        r.sum_b_out[...] += fold(update)
        return cot + joint([dot(pres[n], r.all_t[0, n]) for n in range(quarters)])

    def backward(index, carry):
        cot = r.cot[...]
        for u in range(sizes.unroll):
            cot = retreat(steps - 1 - index * sizes.unroll - u, cot)
        r.cot[...] = cot
        return carry

    lax.fori_loop(0, steps // sizes.unroll, backward, 0)
    for n in range(quarters):
        r.tail[n : n + 1, :] = jnp.sum(r.sum_b_in[n], axis=0, keepdims=True)
    r.tail[quarters : quarters + 1, :] = jnp.sum(r.sum_b_out[...], axis=0, keepdims=True)
    r.tail[quarters + 1 : quarters + 2, :rows] = loglik
    r.tail[quarters + 1 : quarters + 2, rows : 2 * rows] = kl_row
    r.tail[quarters + 2 :, :] = jnp.zeros((r.tail.shape[0] - quarters - 2, width), F32)
    tail_near = send(r.tail, r.tail_sib, r.near, 0, sibling)
    tail_near.start()
    waits = [tail_near]
    leaving = []

    def put(source, target):
        copy = pltpu.make_async_copy(source, target, r.out_sem.at[len(leaving)])
        copy.start()
        leaving.append(copy)

    put(r.elbo, r.elbo_out)
    put(r.cot, r.cot_out)
    dec_grad = dot(r.xt[:, rows:], r.miss[rows:, :])
    dec_grad = dec_grad[:, :seen_width] + dec_grad[:, seen_width:]
    r.dec_part[...] = dec_grad.reshape(r.dec_part.shape)
    dec_near = send(r.dec_part.at[other], r.dec_sib, r.near, 1, sibling)
    dec_near.start()
    waits.append(dec_near)
    dec_rows = r.dec_sum.shape[1]

    def chunk(i, d):
        n = quarter_at(d)
        r.grad[i, 0] = dot(r.xt[:, : steps * rows], r.pre[n])
        r.grad[i, 1] = dot(r.ut[...], r.act[n]).T
        copy = send(r.grad.at[i, other], r.grad_sib.at[i], r.near, 3 + i, sibling)
        copy.start()
        waits.append(copy)
        return copy

    def joined(i, copy):
        copy.wait_recv()
        return r.grad[i, core] + r.grad_sib[i]

    def pass_on(i, d, copy):
        r.line_out[i] = joined(i, copy).astype(BF16)
        send(r.line_out.at[i], r.line_in.at[i], r.line, 0, line_peer(d)).start()

    nears = []
    for i, d in enumerate(far):
        near = chunk(i, d)
        if i == 0:
            tail_near.wait_recv()
            r.tail_sum[...] = r.tail[...] + r.tail_sib[...]
            dec_near.wait_recv()
            r.dec_sum[...] = (r.dec_part[core] + r.dec_sib[...]).reshape(r.dec_sum.shape)
            for e in range(1, planes):
                send(r.tail_sum, r.tail_in.at[e - 1], r.tail_plane, 0, plane_peer(e)).start()
                send(
                    r.dec_sum.at[place_at(e)], r.dec_in.at[e - 1], r.dec_plane, 0, plane_peer(e)
                ).start()
        nears.append(near)
        if i > 0:
            pass_on(i - 1, far[i - 1], nears[i - 1])
    last = len(far)
    near = chunk(last, 0)
    pass_on(last - 1, far[last - 1], nears[last - 1])
    value = r.tail_sum[...]
    arrived(r.tail_in, r.tail_plane)
    for e in range(1, planes):
        value = value + r.tail_in[e - 1]
    r.tail_line[...] = value
    value = r.dec_sum[place]
    arrived(r.dec_in, r.dec_plane)
    for e in range(1, planes):
        value = value + r.dec_in[e - 1]
    r.dec_line[...] = value
    for e in range(1, quarters):
        send(r.tail_line, r.tail_line_in.at[e - 1], r.tail_far, 0, line_peer(e)).start()
        send(r.dec_line, r.dec_line_in.at[e - 1], r.dec_far, 0, line_peer(e)).start()
    value = joined(last, near)
    arrived(r.line_in, r.line)
    for i in range(last):
        value = value + r.line_in[i].astype(F32)
    r.full[...] = value
    r.plane_out[...] = value.astype(BF16).reshape(r.plane_out.shape)
    for e in range(1, planes):
        send(
            r.plane_out.at[place_at(e)], r.plane_in.at[e - 1], r.plane, 0, plane_peer(e)
        ).start()
    piece = width // planes

    def rows_of(tensor, owner):
        return r.res.at[tensor, pl.ds(pl.multiple_of(owner * piece, piece), piece), :]

    value = r.dec_line[...]
    arrived(r.dec_line_in, r.dec_far)
    for e in range(1, quarters):
        value = value + r.dec_line_in[e - 1]
    r.dec_all[core, place] = value / total
    own = r.dec_all.at[core, place]
    for e in range(1, planes):
        send(own, own, r.dec_spread, 0, plane_peer(e)).start()
    value = r.tail_line[...]
    arrived(r.tail_line_in, r.tail_far)
    for e in range(1, quarters):
        value = value + r.tail_line_in[e - 1]
    r.tail_total[...] = value
    scale = 1.0 / total
    r.b_in_sum[...] = r.tail_total[pl.ds(mine, 1), :] * scale
    r.b_out_sum[...] = r.tail_total[quarters : quarters + 1, :] * scale
    points = r.tail_total[quarters + 1 : quarters + 2, :] * scale
    r.scores[:, 0:1] = jnp.sum(points[:, :rows], axis=1, keepdims=True)
    r.scores[:, 1:2] = jnp.sum(points[:, rows : 2 * rows], axis=1, keepdims=True)
    value = r.full[pl.ds(pl.multiple_of(place * piece, piece), piece), :]
    arrived(r.plane_in, r.plane)
    for e in range(1, planes):
        value = value + r.plane_in[e - 1].astype(F32)
    r.res[core, pl.ds(pl.multiple_of(place * piece, piece), piece), :] = value / total
    own = rows_of(core, place)
    for e in range(1, planes):
        send(own, own, r.spread, 0, plane_peer(e)).start()
    arrived(r.dec_all.at[core, pl.ds(0, planes - 1)], r.dec_spread)
    copy = send(r.dec_all.at[core], r.dec_all.at[core], r.near, 2, sibling)
    copy.start()
    waits.append(copy)
    put(r.b_in_sum, r.b_in_out)
    put(r.b_out_sum, r.b_out_out)
    put(r.scores, r.scores_out)
    pieces = pl.ds(0, width - piece)
    arrived(r.res.at[core, pieces], r.spread)
    copy = send(r.res.at[core], r.res.at[core], r.hand, 0, sibling)
    copy.start()
    waits.append(copy)
    got = r.dec_all.at[other]
    send(got, got, r.near, 2, sibling).wait_recv()
    put(r.dec_all, r.dec_out)
    arrived(r.res.at[other], r.hand)
    put(r.res.at[0], r.w_in_out)
    put(r.res.at[1], r.w_out_out)
    departed(r.line_in, r.line)
    departed(r.tail_in, r.tail_plane)
    departed(r.dec_in, r.dec_plane)
    departed(r.tail_line_in, r.tail_far)
    departed(r.dec_line_in, r.dec_far)
    departed(r.dec_all.at[core, pl.ds(0, planes - 1)], r.dec_spread)
    departed(r.plane_in, r.plane)
    departed(r.res.at[core, pieces], r.spread)
    for copy in waits:
        copy.wait_send()
    for copy in leaving:
        copy.wait()


def fused(sizes, operands):
    rows, width, steps = sizes.rows, sizes.width, sizes.steps
    count, seen_width = sizes.seen_count, sizes.seen_width
    quarters, planes = sizes.quarters, sizes.planes
    piece = width // planes
    dec_rows = width // 2 // planes
    outs = {
        "elbo_out": ((1, rows), F32),
        "w_in_out": ((width, width), F32),
        "w_out_out": ((width, width), F32),
        "b_in_out": ((1, width), F32),
        "b_out_out": ((1, width), F32),
        "dec_out": ((2, planes, dec_rows, seen_width), F32),
        "scores_out": ((1, 2), F32),
        "cot_out": ((rows, width), F32),
    }
    arrays = {
        "xt": ((width, (steps + 1) * rows), BF16),
        "ut": ((width, steps * rows), BF16),
        "act": ((quarters, steps * rows, width), BF16),
        "pre": ((quarters, steps * rows, width), BF16),
        "scaled": ((steps, rows, width), F32),
        "pick": ((count, rows, seen_width), F32),
        "obs_wide": ((count, rows, rows), jnp.int32),
        "dt": ((rows, rows), F32),
        "root": ((rows, rows), F32),
        "len": ((rows, rows), jnp.int32),
        "state": ((rows, width), F32),
        "kl": ((rows, width), F32),
        "cot": ((rows, width), F32),
        "ones": ((1, width), F32),
        "sum_b_in": ((quarters, 8, width), F32),
        "sum_b_out": ((8, width), F32),
        "miss": (((steps + 1) * rows, 2 * seen_width), BF16),
        "target": ((rows * count, seen_width), F32),
        "all_w": ((2, quarters, width, width), BF16),
        "all_t": ((2, quarters, width, width), BF16),
        "all_b": ((quarters, 8, width), F32),
        "b_own": (sizes.b_shape, BF16),
        "dec_t": ((2 * seen_width, width), BF16),
        "elbo": ((1, rows), F32),
        "res": ((2, width, width), F32),
        "b_in_sum": ((1, width), F32),
        "b_out_sum": ((1, width), F32),
        "scores": ((1, 2), F32),
        "tail": ((8, width), F32),
        "tail_sib": ((8, width), F32),
        "tail_sum": ((8, width), F32),
        "tail_in": ((planes - 1, 8, width), F32),
        "tail_line": ((8, width), F32),
        "tail_total": ((8, width), F32),
        "tail_line_in": ((quarters - 1, 8, width), F32),
        "dec_part": ((2, width // 2, seen_width), F32),
        "dec_sib": ((width // 2, seen_width), F32),
        "dec_sum": ((planes, dec_rows, seen_width), F32),
        "dec_in": ((planes - 1, dec_rows, seen_width), F32),
        "dec_line": ((dec_rows, seen_width), F32),
        "dec_line_in": ((quarters - 1, dec_rows, seen_width), F32),
        "dec_all": ((2, planes, dec_rows, seen_width), F32),
        "grad": ((quarters, 2, width, width), F32),
        "grad_sib": ((quarters, width, width), F32),
        "line_out": ((quarters - 1, width, width), BF16),
        "line_in": ((quarters - 1, width, width), BF16),
        "full": ((width, width), F32),
        "plane_out": ((planes, piece, width), BF16),
        "plane_in": ((planes - 1, piece, width), BF16),
    }
    for name, value in zip(OPERANDS, operands):
        if name not in ("w_in", "w_out", "b_in"):
            arrays[name] = (value.shape, value.dtype)
    links = {
        "w_far": quarters - 1,
        "w_near": 1,
        "b_far": 1,
        "near": 3 + quarters,
        "line": 1,
        "tail_plane": 1,
        "dec_plane": 1,
        "tail_far": 1,
        "dec_far": 1,
        "dec_spread": 1,
        "plane": 1,
        "spread": 1,
        "hand": 1,
    }
    scratch = [pltpu.VMEM(shape, dtype) for shape, dtype in arrays.values()]
    for number in links.values():
        scratch += [pltpu.SemaphoreType.DMA((number,))] * 2
    scratch.append(pltpu.SemaphoreType.DMA((len(OPERANDS),)))
    scratch.append(pltpu.SemaphoreType.DMA((len(outs),)))

    def body(*refs):
        refs = list(refs)
        r = types.SimpleNamespace()
        for name in OPERANDS:
            setattr(r, name + "_hbm", refs.pop(0))
        for name in list(outs) + list(arrays):
            setattr(r, name, refs.pop(0))
        for name in links:
            setattr(r, name, (refs.pop(0), refs.pop(0)))
        r.load_sem = refs.pop(0)
        r.out_sem = refs.pop(0)
        fused_kernel(sizes, r)

    return pl.pallas_call(
        body,
        out_shape=[jax.ShapeDtypeStruct(shape, dtype) for shape, dtype in outs.values()],
        in_specs=[pl.BlockSpec(memory_space=pltpu.HBM)] * len(OPERANDS),
        out_specs=[pl.BlockSpec(memory_space=pltpu.HBM)] * len(outs),
        scratch_shapes=scratch,
        compiler_params=pltpu.CompilerParams(
            collective_id=0, has_side_effects=True, vmem_limit_bytes=60 * 1024 * 1024
        ),
        name="fused",
    )(*operands)


def finish(arrays):
    number = len(arrays)

    def body(*refs):
        ins, outs, spaces = refs[:number], refs[number : 2 * number], refs[2 * number : 3 * number]
        taken, given = refs[3 * number :]
        loads = [
            pltpu.make_async_copy(source, space, taken.at[i])
            for i, (source, space) in enumerate(zip(ins, spaces))
        ]
        stores = [
            pltpu.make_async_copy(space, target, given.at[i])
            for i, (space, target) in enumerate(zip(spaces, outs))
        ]
        for load in loads:
            load.start()
        for load, store in zip(loads, stores):
            load.wait()
            store.start()
        for store in stores:
            store.wait()

    hbm = pl.BlockSpec(memory_space=pltpu.HBM)
    return pl.pallas_call(
        body,
        out_shape=[jax.ShapeDtypeStruct(value.shape, value.dtype) for value in arrays],
        in_specs=[hbm] * number,
        out_specs=[hbm] * number,
        scratch_shapes=[pltpu.VMEM(value.shape, value.dtype) for value in arrays]
        + [pltpu.SemaphoreType.DMA((number,))] * 2,
        compiler_params=pltpu.CompilerParams(vmem_limit_bytes=60 * 1024 * 1024),
        name="finish",
    )(*arrays)


def on_device(
    init_state,
    brownian,
    step_size,
    lengths,
    obs_steps,
    observed,
    w_in,
    b_in,
    w_out,
    b_out,
    decoder,
    prior_rate,
    diffusion,
):
    rows, width = init_state.shape
    quarters = lax.axis_size("mp")
    members = lax.axis_size("batch")
    sizes = types.SimpleNamespace(
        rows=rows,
        width=width,
        steps=brownian.shape[0],
        seen_count=observed.shape[1],
        seen_width=observed.shape[2],
        quarters=quarters,
        planes=members // 2,
        total=rows * members * quarters,
        unroll=UNROLL,
        b_shape=b_in.shape,
    )
    results = fused(
        sizes,
        (
            init_state,
            brownian,
            step_size[None, :],
            lengths[None, :],
            obs_steps.T,
            observed,
            w_in,
            b_in,
            w_out,
            b_out[None, :],
            decoder,
            prior_rate[None, :],
            diffusion[None, :],
        ),
    )
    elbo, own_w_in, own_w_out, own_b_in, b_out_grad, dec_grad, scores, cot = finish(results)
    dec_grad = dec_grad.reshape(decoder.shape)
    return (
        elbo[0],
        scores[0],
        own_w_in,
        own_b_in[0],
        own_w_out,
        b_out_grad[0],
        dec_grad,
        cot,
    )


def solution(mesh):
    both = ("batch", "mp")
    placed = (
        P(both, None),
        P(None, both, None),
        P(both),
        P(both),
        P(both, None),
        P(both, None, None),
        P(None, "mp"),
        P("mp"),
        P("mp", None),
        P(),
        P(),
        P(),
        P(),
    )
    return jax.shard_map(
        on_device,
        mesh=mesh,
        in_specs=placed,
        out_specs=(
            P(both),
            P(),
            P(None, "mp"),
            P("mp"),
            P("mp", None),
            P(),
            P(),
            P(both, None),
        ),
        check_vma=False,
    )
```
